1024 devices in a mesh: gx: 4 (over y), gy: 4 (over z_hi), gz: 64 (over x, z_lo, core).
Axes of the slice: x: 4, y: 4, z: 32 (z_hi: 4, z_lo: 8; z = z_hi * 8 + z_lo), core: 2. Of those that a mesh axis runs over, the one named last changes fastest.
Arguments:
- section: float32 [25, 128, 64, 512], P(None, 'gz', 'gy', 'gx'), may hold values from -0.4 to 1.4, as said below
- base: float32 [25, 128, 64, 512], P(None, 'gz', 'gy', 'gx'), may hold values from -0.4 to 1.4, as said below
- accum: float32 [25, 128, 64, 512], P(None, 'gz', 'gy', 'gx'), may hold values from -4 to 4
Outputs:
- next_section: float32 [25, 128, 64, 512], P(None, 'gz', 'gy', 'gx')
- next_accum: float32 [25, 128, 64, 512], P(None, 'gz', 'gy', 'gx')
- slab: float32 [25, 128, 64, 512], P(None, 'gz')
The draws below stay inside these ranges and needn't reach their ends.
Inputs may be any that keep to these rules, and one draw needn't show every extreme that they name: `section`: fields 0 and 17 (conformal factor and lapse) lie in 0.6 to 1.4; fields 1, 4 and 6 (the metric's diagonal) lie within 0.4 of 1; all other fields lie within 0.4 of 0. `base`: fields 0 and 17 (conformal factor and lapse) lie in 0.6 to 1.4; fields 1, 4 and 6 (the metric's diagonal) lie within 0.4 of 1; all other fields lie within 0.4 of 0.
All inputs are finite; a program needn't handle non-finite values.
Results may differ from the reference program's by a relative error of at most 0.0003.
Values sent between devices are 32-bit elements; how exact they have to be, the bound alone decides.
No kernel may reach another device: no remote copies, remote signals or barrier semaphores. Data moves between devices by JAX's collectives and lax.ppermute only.
A program may use at most 64 MiB of HBM per device.

```python
import jax
import jax.numpy as jnp
from jax import lax

FIELDS = 25
CZ = 2
NZ = 128
NY = 64
NX = 512
N_GZ = 64


def draw_fields(key):
    subkeys = jax.random.split(key, 2)
    full_shape = (FIELDS, NZ, NY, NX)
    jitter = jnp.clip(0.1 * jax.random.normal(subkeys[0], full_shape, jnp.float32), -0.4, 0.4)
    positive = 1.0 + jnp.clip(0.15 * jax.random.normal(subkeys[1], full_shape, jnp.float32), -0.4, 0.4)
    field_slot = lax.broadcasted_iota(jnp.int32, full_shape, 0)
    unit_diag = (field_slot == 1) | (field_slot == 4) | (field_slot == 6)
    kept_positive = (field_slot == 0) | (field_slot == 17)
    values = jnp.where(unit_diag, 1.0 + jitter, jitter)
    return jnp.where(kept_positive, positive, values)


def draw_section(key, part):
    return draw_fields(jax.random.fold_in(key, 11))


def draw_base(key, part):
    return draw_fields(jax.random.fold_in(key, 23))


def shard_levels(key, dims, shards, smallest, high):
    gain, own = 1.0, jax.random.fold_in(key, 6)
    for dim, blocks in shards:
        steps = jnp.exp(jax.random.uniform(jax.random.fold_in(own, dim), (blocks,), jnp.float32, smallest / len(shards), high / len(shards)))
        gain = gain * jnp.repeat(steps, dims[dim] // blocks).reshape([-1 if axis == dim else 1 for axis in range(len(dims))])
    return gain


def centred(rng, shape, spread, reach, pieces=(), held_as=jnp.bfloat16):
    entries = jax.random.normal(rng, shape, jnp.float32) * spread
    if len(pieces) > 0:
        entries = shard_levels(rng, shape, pieces, -0.22, 0.18) * entries
    return jnp.clip(entries, min=-reach, max=reach).astype(held_as)


def setup_inputs(seed: int = 0) -> dict:
    streams_of = jax.random.split(jax.random.key(seed), 4)
    section = draw_section(jax.random.fold_in(streams_of[3], 71), 0)
    base = draw_base(jax.random.fold_in(streams_of[3], 71), 0)
    accum = centred(streams_of[2], (FIELDS, NZ, NY, NX), 0.5, 4.0, ((1, 64), (2, 4), (3, 4)), jnp.float32)
    return dict(section=section, base=base, accum=accum)


STEP_DT = 0.25
SPACING = 1.0
DISSIPATE = 0.1
DRIVER_ETA = 2.0
KAPPA_ONE = 0.1
FIRST_TAPS = (1.0 / 12.0, -8.0 / 12.0, 0.0, 8.0 / 12.0, -1.0 / 12.0)
SECOND_TAPS = (-1.0 / 12.0, 16.0 / 12.0, -30.0 / 12.0, 16.0 / 12.0, -1.0 / 12.0)
FOURTH_TAPS = (1.0, -4.0, 6.0, -4.0, 1.0)
PAIR_SLOT = ((0, 1, 2), (1, 3, 4), (2, 4, 5))
PAIR_LIST = ((0, 0), (0, 1), (0, 2), (1, 1), (1, 2), (2, 2))


def window(padded, shifts):
    interior = (padded.shape[1] - 4, padded.shape[2] - 4, padded.shape[3] - 4)
    corner = (2 + shifts[2], 2 + shifts[1], 2 + shifts[0])
    return padded[:, corner[0]:corner[0] + interior[0], corner[1]:corner[1] + interior[1], corner[2]:corner[2] + interior[2]]


def moved(direction, amount):
    shifts = [0, 0, 0]
    shifts[direction] = amount
    return shifts


def line_sum(padded, direction, weights):
    running = None
    for position in range(5):
        if weights[position] != 0.0:
            weighted = weights[position] * window(padded, moved(direction, position - 2))
            running = weighted if running is None else running + weighted
    return running


def cross_sum(padded, first_dir, second_dir):
    running = None
    for first_pos in range(5):
        for second_pos in range(5):
            factor = FIRST_TAPS[first_pos] * FIRST_TAPS[second_pos]
            if factor != 0.0:
                shifts = [0, 0, 0]
                shifts[first_dir] = first_pos - 2
                shifts[second_dir] = second_pos - 2
                weighted = factor * window(padded, shifts)
                running = weighted if running is None else running + weighted
    return running


def evolve_rate(padded):
    centre = window(padded, (0, 0, 0))
    gradients = [line_sum(padded, direction, FIRST_TAPS) / SPACING for direction in range(3)]
    curves = [line_sum(padded, direction, SECOND_TAPS) / (SPACING * SPACING) for direction in range(3)]
    smoothing = line_sum(padded, 0, FOURTH_TAPS) + line_sum(padded, 1, FOURTH_TAPS) + line_sum(padded, 2, FOURTH_TAPS)
    chosen = jnp.concatenate([padded[0:1], padded[17:21]], axis=0)
    mixed_terms = {}
    for dir_pair in ((0, 1), (0, 2), (1, 2)):
        mixed_terms[dir_pair] = cross_sum(chosen, dir_pair[0], dir_pair[1]) / (SPACING * SPACING)

    def second_of(chosen_slot, field_slot, axis_one, axis_two):
        if axis_one == axis_two:
            return curves[axis_one][field_slot]
        return mixed_terms[(min(axis_one, axis_two), max(axis_one, axis_two))][chosen_slot]

    def metric_of(axis_one, axis_two):
        return centre[1 + PAIR_SLOT[axis_one][axis_two]]

    def traceless_of(axis_one, axis_two):
        return centre[8 + PAIR_SLOT[axis_one][axis_two]]

    def inverse_of(axis_one, axis_two):
        return (2.0 if axis_one == axis_two else 0.0) - metric_of(axis_one, axis_two)

    def advect(field_slot):
        return centre[18] * gradients[0][field_slot] + centre[19] * gradients[1][field_slot] + centre[20] * gradients[2][field_slot]

    conformal = centre[0]
    trace_curv = centre[7]
    lapse_field = centre[17]
    theta_field = centre[24]
    divergence = gradients[0][18] + gradients[1][19] + gradients[2][20]
    lap_conformal = curves[0][0] + curves[1][0] + curves[2][0]
    squares_a = sum(traceless_of(axis_one, axis_two) ** 2 for axis_one in range(3) for axis_two in range(3))

    def lapse_dd(axis_one, axis_two):
        return second_of(1, 17, axis_one, axis_two)

    ricci_table = []
    for axis_one, axis_two in PAIR_LIST:
        field_slot = 1 + PAIR_SLOT[axis_one][axis_two]
        flat_part = curves[0][field_slot] + curves[1][field_slot] + curves[2][field_slot]
        conformal_part = second_of(0, 0, axis_one, axis_two) + (lap_conformal if axis_one == axis_two else 0.0)
        ricci_table.append(-0.5 * flat_part + 0.5 * (gradients[axis_one][14 + axis_two] + gradients[axis_two][14 + axis_one]) + conformal_part / (2.0 * conformal))

    def ricci_of(axis_one, axis_two):
        return ricci_table[PAIR_SLOT[axis_one][axis_two]]

    ricci_scalar = conformal * sum(inverse_of(axis_one, axis_two) * ricci_of(axis_one, axis_two) for axis_one in range(3) for axis_two in range(3))
    lapse_trace = sum(inverse_of(axis_one, axis_two) * lapse_dd(axis_one, axis_two) for axis_one in range(3) for axis_two in range(3))

    rates = [None] * 25
    rates[0] = advect(0) + (2.0 / 3.0) * conformal * (lapse_field * trace_curv - divergence)
    for axis_one, axis_two in PAIR_LIST:
        field_slot = PAIR_SLOT[axis_one][axis_two]
        lie_part = sum(metric_of(axis_one, axis_sum) * gradients[axis_two][18 + axis_sum] + metric_of(axis_two, axis_sum) * gradients[axis_one][18 + axis_sum] for axis_sum in range(3))
        rates[1 + field_slot] = advect(1 + field_slot) - 2.0 * lapse_field * traceless_of(axis_one, axis_two) + lie_part - (2.0 / 3.0) * metric_of(axis_one, axis_two) * divergence
    rates[7] = advect(7) - conformal * lapse_trace + lapse_field * (squares_a + trace_curv * trace_curv / 3.0) + KAPPA_ONE * lapse_field * theta_field

    def source_of(axis_one, axis_two):
        return -lapse_dd(axis_one, axis_two) + lapse_field * ricci_of(axis_one, axis_two)

    trace_part = sum(inverse_of(axis_one, axis_two) * source_of(axis_one, axis_two) for axis_one in range(3) for axis_two in range(3))
    for axis_one, axis_two in PAIR_LIST:
        field_slot = PAIR_SLOT[axis_one][axis_two]
        free_part = source_of(axis_one, axis_two) - metric_of(axis_one, axis_two) * trace_part / 3.0
        product_part = sum(traceless_of(axis_one, axis_sum) * traceless_of(axis_sum, axis_two) for axis_sum in range(3))
        lie_part = sum(traceless_of(axis_one, axis_sum) * gradients[axis_two][18 + axis_sum] + traceless_of(axis_two, axis_sum) * gradients[axis_one][18 + axis_sum] for axis_sum in range(3))
        rates[8 + field_slot] = (advect(8 + field_slot) + conformal * free_part
                                 + lapse_field * (trace_curv * traceless_of(axis_one, axis_two) - 2.0 * product_part)
                                 + lie_part - (2.0 / 3.0) * traceless_of(axis_one, axis_two) * divergence)
    for axis_one in range(3):
        gauge_part = (-2.0 * sum(traceless_of(axis_one, axis_two) * gradients[axis_two][17] for axis_two in range(3))
                      + 2.0 * lapse_field * (-(2.0 / 3.0) * sum(inverse_of(axis_one, axis_two) * gradients[axis_two][7] for axis_two in range(3))
                                             - 1.5 * sum(traceless_of(axis_one, axis_two) * gradients[axis_two][0] for axis_two in range(3)) / conformal)
                      + curves[0][18 + axis_one] + curves[1][18 + axis_one] + curves[2][18 + axis_one]
                      + sum(second_of(2 + axis_two, 18 + axis_two, axis_one, axis_two) for axis_two in range(3)) / 3.0
                      + (2.0 / 3.0) * centre[14 + axis_one] * divergence
                      - sum(centre[14 + axis_two] * gradients[axis_two][18 + axis_one] for axis_two in range(3)))
        rates[14 + axis_one] = advect(14 + axis_one) + gauge_part
        rates[18 + axis_one] = advect(18 + axis_one) + 0.75 * centre[21 + axis_one]
        rates[21 + axis_one] = advect(21 + axis_one) + gauge_part - DRIVER_ETA * centre[21 + axis_one]
    rates[17] = advect(17) - 2.0 * lapse_field * (trace_curv - 2.0 * theta_field)
    rates[24] = (advect(24) + 0.5 * lapse_field * (ricci_scalar + (2.0 / 3.0) * trace_curv * trace_curv - squares_a)
                 - 2.0 * KAPPA_ONE * lapse_field * theta_field)
    return jnp.stack(rates, axis=0) + (-DISSIPATE / 16.0) * smoothing


def reference(section, base, accum):
    padded = jnp.pad(section, ((0, 0), (2, 2), (2, 2), (2, 2)), mode="wrap")

    def one_block(block_index):
        start_plane = (block_index * CZ).astype(jnp.int32)
        piece_block = lax.dynamic_slice_in_dim(padded, start_plane, CZ + 4, 1)
        return evolve_rate(piece_block)

    blocks = lax.map(one_block, jnp.arange(N_GZ, dtype=jnp.int32))
    rates = jnp.moveaxis(blocks, 0, 1).reshape(FIELDS, NZ, NY, NX)
    next_section = base + (0.5 * STEP_DT) * rates
    next_accum = accum + (STEP_DT / 3.0) * rates
    return next_section, next_accum, next_section
```

```python
import jax
import jax.numpy as jnp
from jax import lax
from jax.experimental import pallas as pl
from jax.experimental.pallas import tpu as pltpu
from jax.sharding import PartitionSpec as P


STEP_DT = 0.25
SPACING = 1.0
DISSIPATE = 0.1
DRIVER_ETA = 2.0
KAPPA_ONE = 0.1
FIRST_TAPS = (1.0 / 12.0, -8.0 / 12.0, 0.0, 8.0 / 12.0, -1.0 / 12.0)
SECOND_TAPS = (-1.0 / 12.0, 16.0 / 12.0, -30.0 / 12.0, 16.0 / 12.0, -1.0 / 12.0)
FOURTH_TAPS = (1.0, -4.0, 6.0, -4.0, 1.0)
PAIR_SLOT = ((0, 1, 2), (1, 3, 4), (2, 4, 5))
PAIR_LIST = ((0, 0), (0, 1), (0, 2), (1, 1), (1, 2), (2, 2))


def extended(block, sides, width):
    for axis, dim in sides:
        count = lax.axis_size(axis)
        forward = [(i, i + 1) for i in range(count - 1)]
        forward.append((count - 1, 0))
        backward = [(target, source) for source, target in forward]
        low = lax.ppermute(
            lax.slice_in_dim(block, block.shape[dim] - width, None, axis=dim), axis, forward
        )
        high = lax.ppermute(lax.slice_in_dim(block, 0, width, axis=dim), axis, backward)
        block = jnp.concatenate([low, block, high], axis=dim)
    return block


def window(padded, shifts):
    interior = (padded.shape[1] - 4, padded.shape[2] - 4, padded.shape[3] - 4)
    corner = (2 + shifts[2], 2 + shifts[1], 2 + shifts[0])
    return padded[
        :,
        corner[0] : corner[0] + interior[0],
        corner[1] : corner[1] + interior[1],
        corner[2] : corner[2] + interior[2],
    ]


def moved(direction, amount):
    shifts = [0, 0, 0]
    shifts[direction] = amount
    return shifts


def line_sum(padded, direction, weights):
    running = None
    for position in range(5):
        if weights[position] != 0.0:
            weighted = weights[position] * window(padded, moved(direction, position - 2))
            running = weighted if running is None else running + weighted
    return running


def cross_sum(padded, first_dir, second_dir):
    running = None
    for first_pos in range(5):
        for second_pos in range(5):
            factor = FIRST_TAPS[first_pos] * FIRST_TAPS[second_pos]
            if factor != 0.0:
                shifts = [0, 0, 0]
                shifts[first_dir] = first_pos - 2
                shifts[second_dir] = second_pos - 2
                weighted = factor * window(padded, shifts)
                running = weighted if running is None else running + weighted
    return running


def evolve_rate(padded):
    centre = window(padded, (0, 0, 0))
    gradients = [line_sum(padded, direction, FIRST_TAPS) / SPACING for direction in range(3)]
    curves = [
        line_sum(padded, direction, SECOND_TAPS) / (SPACING * SPACING) for direction in range(3)
    ]
    smoothing = (
        line_sum(padded, 0, FOURTH_TAPS)
        + line_sum(padded, 1, FOURTH_TAPS)
        + line_sum(padded, 2, FOURTH_TAPS)
    )
    chosen = jnp.concatenate([padded[0:1], padded[17:21]], axis=0)
    mixed_terms = {}
    for dir_pair in ((0, 1), (0, 2), (1, 2)):
        mixed_terms[dir_pair] = cross_sum(chosen, dir_pair[0], dir_pair[1]) / (SPACING * SPACING)

    def second_of(chosen_slot, field_slot, axis_one, axis_two):
        if axis_one == axis_two:
            return curves[axis_one][field_slot]
        return mixed_terms[min(axis_one, axis_two), max(axis_one, axis_two)][chosen_slot]

    def metric_of(axis_one, axis_two):
        return centre[1 + PAIR_SLOT[axis_one][axis_two]]

    def traceless_of(axis_one, axis_two):
        return centre[8 + PAIR_SLOT[axis_one][axis_two]]

    def inverse_of(axis_one, axis_two):
        return (2.0 if axis_one == axis_two else 0.0) - metric_of(axis_one, axis_two)

    def advect(field_slot):
        return (
            centre[18] * gradients[0][field_slot]
            + centre[19] * gradients[1][field_slot]
            + centre[20] * gradients[2][field_slot]
        )

    conformal = centre[0]
    trace_curv = centre[7]
    lapse_field = centre[17]
    theta_field = centre[24]
    divergence = gradients[0][18] + gradients[1][19] + gradients[2][20]
    lap_conformal = curves[0][0] + curves[1][0] + curves[2][0]
    squares_a = sum(
        (traceless_of(axis_one, axis_two) ** 2 for axis_one in range(3) for axis_two in range(3))
    )

    def lapse_dd(axis_one, axis_two):
        return second_of(1, 17, axis_one, axis_two)

    ricci_table = []
    for axis_one, axis_two in PAIR_LIST:
        field_slot = 1 + PAIR_SLOT[axis_one][axis_two]
        flat_part = curves[0][field_slot] + curves[1][field_slot] + curves[2][field_slot]
        conformal_part = second_of(0, 0, axis_one, axis_two) + (
            lap_conformal if axis_one == axis_two else 0.0
        )
        ricci_table.append(
            -0.5 * flat_part
            + 0.5 * (gradients[axis_one][14 + axis_two] + gradients[axis_two][14 + axis_one])
            + conformal_part / (2.0 * conformal)
        )

    def ricci_of(axis_one, axis_two):
        return ricci_table[PAIR_SLOT[axis_one][axis_two]]

    ricci_scalar = conformal * sum(
        (
            inverse_of(axis_one, axis_two) * ricci_of(axis_one, axis_two)
            for axis_one in range(3)
            for axis_two in range(3)
        )
    )
    lapse_trace = sum(
        (
            inverse_of(axis_one, axis_two) * lapse_dd(axis_one, axis_two)
            for axis_one in range(3)
            for axis_two in range(3)
        )
    )
    rates = [None] * 25
    rates[0] = advect(0) + 2.0 / 3.0 * conformal * (lapse_field * trace_curv - divergence)
    for axis_one, axis_two in PAIR_LIST:
        field_slot = PAIR_SLOT[axis_one][axis_two]
        lie_part = sum(
            (
                metric_of(axis_one, axis_sum) * gradients[axis_two][18 + axis_sum]
                + metric_of(axis_two, axis_sum) * gradients[axis_one][18 + axis_sum]
                for axis_sum in range(3)
            )
        )
        rates[1 + field_slot] = (
            advect(1 + field_slot)
            - 2.0 * lapse_field * traceless_of(axis_one, axis_two)
            + lie_part
            - 2.0 / 3.0 * metric_of(axis_one, axis_two) * divergence
        )
    rates[7] = (
        advect(7)
        - conformal * lapse_trace
        + lapse_field * (squares_a + trace_curv * trace_curv / 3.0)
        + KAPPA_ONE * lapse_field * theta_field
    )

    def source_of(axis_one, axis_two):
        return -lapse_dd(axis_one, axis_two) + lapse_field * ricci_of(axis_one, axis_two)

    trace_part = sum(
        (
            inverse_of(axis_one, axis_two) * source_of(axis_one, axis_two)
            for axis_one in range(3)
            for axis_two in range(3)
        )
    )
    for axis_one, axis_two in PAIR_LIST:
        field_slot = PAIR_SLOT[axis_one][axis_two]
        free_part = source_of(axis_one, axis_two) - metric_of(axis_one, axis_two) * trace_part / 3.0
        product_part = sum(
            (
                traceless_of(axis_one, axis_sum) * traceless_of(axis_sum, axis_two)
                for axis_sum in range(3)
            )
        )
        lie_part = sum(
            (
                traceless_of(axis_one, axis_sum) * gradients[axis_two][18 + axis_sum]
                + traceless_of(axis_two, axis_sum) * gradients[axis_one][18 + axis_sum]
                for axis_sum in range(3)
            )
        )
        rates[8 + field_slot] = (
            advect(8 + field_slot)
            + conformal * free_part
            + lapse_field * (trace_curv * traceless_of(axis_one, axis_two) - 2.0 * product_part)
            + lie_part
            - 2.0 / 3.0 * traceless_of(axis_one, axis_two) * divergence
        )
    for axis_one in range(3):
        gauge_part = (
            -2.0
            * sum(
                (
                    traceless_of(axis_one, axis_two) * gradients[axis_two][17]
                    for axis_two in range(3)
                )
            )
            + 2.0
            * lapse_field
            * (
                -(2.0 / 3.0)
                * sum(
                    (
                        inverse_of(axis_one, axis_two) * gradients[axis_two][7]
                        for axis_two in range(3)
                    )
                )
                - 1.5
                * sum(
                    (
                        traceless_of(axis_one, axis_two) * gradients[axis_two][0]
                        for axis_two in range(3)
                    )
                )
                / conformal
            )
            + curves[0][18 + axis_one]
            + curves[1][18 + axis_one]
            + curves[2][18 + axis_one]
            + sum(
                (
                    second_of(2 + axis_two, 18 + axis_two, axis_one, axis_two)
                    for axis_two in range(3)
                )
            )
            / 3.0
            + 2.0 / 3.0 * centre[14 + axis_one] * divergence
            - sum(
                (
                    centre[14 + axis_two] * gradients[axis_two][18 + axis_one]
                    for axis_two in range(3)
                )
            )
        )
        rates[14 + axis_one] = advect(14 + axis_one) + gauge_part
        rates[18 + axis_one] = advect(18 + axis_one) + 0.75 * centre[21 + axis_one]
        rates[21 + axis_one] = (
            advect(21 + axis_one) + gauge_part - DRIVER_ETA * centre[21 + axis_one]
        )
    rates[17] = advect(17) - 2.0 * lapse_field * (trace_curv - 2.0 * theta_field)
    rates[24] = (
        advect(24)
        + 0.5 * lapse_field * (ricci_scalar + 2.0 / 3.0 * trace_curv * trace_curv - squares_a)
        - 2.0 * KAPPA_ONE * lapse_field * theta_field
    )
    return jnp.stack(rates, axis=0) + -DISSIPATE / 16.0 * smoothing


AXES = ("gx", "gy", "gz")
N_GX = 4
N_GY = 4


def turned(axis, sense):
    pairs = []
    size_z = lax.axis_size("gz")
    for col in range(N_GX):
        for row in range(N_GY):
            for deep in range(size_z):
                step = sense if deep % 2 == 0 else -sense
                to_col = (col + step) % N_GX if axis == "gx" else col
                to_row = (row + step) % N_GY if axis == "gy" else row
                pairs.append(
                    ((col * N_GY + row) * size_z + deep, (to_col * N_GY + to_row) * size_z + deep)
                )
    return pairs


def place_kernel(step_y, *refs):
    own, first, second, back, slab, sems = refs[0], refs[1], refs[2], refs[3], refs[-2], refs[-1]
    sense = 1 - 2 * lax.rem(lax.axis_index("gz"), 2)
    row = lax.rem(lax.axis_index("gy") - sense * step_y + 2 * N_GY, N_GY)
    height, width = own.shape[2], own.shape[3]
    copies = []
    for number, (piece, away) in enumerate(((own, 0), (first, 1), (second, 2), (back, -1))):
        col = lax.rem(lax.axis_index("gx") - sense * away + 2 * N_GX, N_GX)
        copies.append(
            pltpu.make_async_copy(
                piece,
                slab.at[
                    :,
                    :,
                    pl.ds(pl.multiple_of(row * height, height), height),
                    pl.ds(pl.multiple_of(col * width, width), width),
                ],
                sems.at[number],
            )
        )
    for copy in copies:
        copy.start()
    for copy in copies:
        copy.wait()


def placed(slab, pieces, step_y):
    fields_count, planes, height, width = pieces[0].shape
    shape = jax.ShapeDtypeStruct((fields_count, planes, N_GY * height, N_GX * width), jnp.float32)
    args = list(pieces)
    specs = [pl.BlockSpec(memory_space=pltpu.VMEM)] * 4
    aliases = {}
    if slab is not None:
        args.append(slab)
        specs.append(pl.BlockSpec(memory_space=pl.ANY))
        aliases = {4: 0}
    return pl.pallas_call(
        lambda *refs: place_kernel(step_y, *refs),
        out_shape=shape,
        in_specs=specs,
        out_specs=pl.BlockSpec(memory_space=pl.ANY),
        scratch_shapes=[pltpu.SemaphoreType.DMA((4,))],
        input_output_aliases=aliases,
        cost_estimate=pl.CostEstimate(flops=2000000, bytes_accessed=3300000, transcendentals=0),
        compiler_params=pltpu.CompilerParams(vmem_limit_bytes=4 * 1024 * 1024),
    )(*args)


def slab_of(block):
    along_y = turned("gy", 1)
    along_x = turned("gx", 1)
    against_x = turned("gx", -1)
    slab = None
    current = block
    for step in range(4):
        following = None
        if step < 3:
            following = lax.ppermute(current, AXES, along_y)
        first = lax.ppermute(current, AXES, along_x)
        back = lax.ppermute(current, AXES, against_x)
        second = lax.ppermute(first, AXES, along_x)
        if following is not None:
            following, first, second, back = lax.optimization_barrier(
                (following, first, second, back)
            )
        slab = placed(slab, (current, first, second, back), step)
        current = following
    return slab


def shards(section, base, accum):
    padded = extended(section, (("gx", 3), ("gy", 2), ("gz", 1)), 2)
    rates = evolve_rate(padded)
    next_section = base + 0.5 * STEP_DT * rates
    next_accum = accum + STEP_DT / 3.0 * rates
    return (next_section, next_accum, slab_of(next_section))


def solution(mesh):
    split = P(None, "gz", "gy", "gx")
    return jax.shard_map(
        shards,
        mesh=mesh,
        in_specs=(split, split, split),
        out_specs=(split, split, P(None, "gz", None, None)),
        check_vma=False,
    )
```

```python
import jax
import jax.numpy as jnp
from jax import lax
from jax.experimental import pallas as pl
from jax.experimental.pallas import tpu as pltpu
from jax.sharding import PartitionSpec as P


STEP_DT = 0.25
DISSIPATE = 0.1
DRIVER_ETA = 2.0
KAPPA_ONE = 0.1
PAIR_SLOT = ((0, 1, 2), (1, 3, 4), (2, 4, 5))
PAIR_LIST = ((0, 0), (0, 1), (0, 2), (1, 1), (1, 2), (2, 2))


EDGED = (0, 17, 18, 19, 20)
PAD = 8


def rolled(tile, amount):
    amount = amount % 128
    return tile if amount == 0 else pltpu.roll(tile, amount, 1)


def lanes_of(tile):
    return lax.broadcasted_iota(jnp.int32, tile.shape, 1)


def pack_kernel(section, left, right, top, bottom):
    fields_count, planes, rows, cols = section.shape
    low = jnp.zeros((rows, cols), jnp.float32)
    high = jnp.zeros((rows, cols), jnp.float32)
    lane_pair = lanes_of(low) // 2
    for field in range(fields_count):
        for plane in range(planes):
            number = field * planes + plane
            tile = section[field, plane]
            low = jnp.where(lane_pair == number, rolled(tile, 2 * number), low)
            high = jnp.where(lane_pair == number, rolled(tile, 2 * number + 2), high)
            top[2 * number : 2 * number + 2, :] = section[field, plane, 0:2, :]
            bottom[2 * number : 2 * number + 2, :] = section[field, plane, rows - 2 : rows, :]
    left[...] = low
    right[...] = high


def edge_kernel(from_left, from_right, from_low, from_high, edges, left, right):
    edges[0:16, :] = from_left[...]
    edges[16:32, :] = from_right[...]
    for side, rows in enumerate((from_low, from_high)):
        low = jnp.zeros((2, 128), jnp.float32)
        high = jnp.zeros((2, 128), jnp.float32)
        lane_pair = lanes_of(low) // 2
        for slot, field in enumerate(EDGED):
            for plane in range(2):
                number = slot * 2 + plane
                tile = rows[4 * field + 2 * plane : 4 * field + 2 * plane + 2, :]
                place = 32 + 20 * side + 2 * number
                edges[place : place + 2, :] = tile
                low = jnp.where(lane_pair == number, rolled(tile, 2 * number), low)
                high = jnp.where(lane_pair == number, rolled(tile, 2 * number + 2), high)
        left[2 * side : 2 * side + 2, :] = low
        right[2 * side : 2 * side + 2, :] = high


def border(from_left, from_right, number):
    return jnp.where(
        lanes_of(from_left) >= 64,
        rolled(from_left, 126 - 2 * number),
        rolled(from_right, 128 - 2 * number),
    )


def along_lanes(tile, edge):
    lane = lanes_of(tile)
    return (
        rolled(jnp.where(lane >= 126, edge, tile), 2),
        rolled(jnp.where(lane == 127, edge, tile), 1),
        rolled(jnp.where(lane == 0, edge, tile), 127),
        rolled(jnp.where(lane <= 1, edge, tile), 126),
    )


def slope(around):
    back2, back1, ahead1, ahead2 = around
    return (8.0 / 12.0) * (ahead1 - back1) - (1.0 / 12.0) * (ahead2 - back2)


def rate_kernel(
    section,
    below,
    above,
    from_left,
    from_right,
    from_low,
    from_high,
    edges_below,
    edges_above,
    corner_left,
    corner_right,
    base,
    accum,
    next_section,
    next_accum,
    ext,
    cross_x,
    cross_y,
):
    fields_count, planes, rows, _ = section.shape
    last = PAD + rows
    for field in range(fields_count):
        for plane in range(planes):
            number = 2 * (field * planes + plane)
            ext[field, plane, PAD:last, :] = section[field, plane]
            ext[field, plane, PAD - 2 : PAD, :] = from_low[number : number + 2, :]
            ext[field, plane, last : last + 2, :] = from_high[number : number + 2, :]

    def layer(field, plane):
        if plane < 0:
            return below[field, plane + 2]
        if plane > 1:
            return above[field, plane - 2]
        return section[field, plane]

    for slot, field in enumerate(EDGED):
        for plane in range(-2, 4):
            tile = layer(field, plane)
            if plane in (0, 1):
                edge = border(from_left[...], from_right[...], 2 * field + plane)
                cross_x[slot, plane + 2, PAD:last, :] = slope(along_lanes(tile, edge))
                for side, place in enumerate((PAD - 2, last)):
                    strip = ext[field, plane, place : place + 2, :]
                    edge = border(
                        corner_left[2 * side : 2 * side + 2, :],
                        corner_right[2 * side : 2 * side + 2, :],
                        2 * slot + plane,
                    )
                    cross_x[slot, plane + 2, place : place + 2, :] = slope(
                        along_lanes(strip, edge)
                    )
                column = ext.at[field, plane]
            else:
                source, local = (edges_below, plane + 2) if plane < 0 else (edges_above, plane - 2)
                edge = border(source[0:16, :], source[16:32, :], 2 * field + local)
                cross_x[slot, plane + 2, PAD:last, :] = slope(along_lanes(tile, edge))
                place = 4 * slot + 2 * local
                depth = fields_count + (plane + 2 if plane < 0 else plane)
                column = ext.at[depth, slot % 2]
                column[PAD:last, :] = tile
                column[PAD - 2 : PAD, :] = source[32 + place : 34 + place, :]
                column[last : last + 2, :] = source[52 + place : 54 + place, :]
            cross_y[slot, plane + 2] = slope(
                tuple(column[PAD + off : last + off, :] for off in (-2, -1, 1, 2))
            )

    for plane in range(planes):
        write_rates(
            plane,
            section,
            layer,
            from_left,
            from_right,
            base,
            accum,
            next_section,
            next_accum,
            ext,
            cross_x,
            cross_y,
        )


def write_rates(
    plane,
    section,
    layer,
    from_left,
    from_right,
    base,
    accum,
    next_section,
    next_accum,
    ext,
    cross_x,
    cross_y,
):
    rows = section.shape[2]
    last = PAD + rows
    centre = [section[field, plane] for field in range(25)]
    gradients = [[None] * 25 for _ in range(3)]
    curves = [[None] * 25 for _ in range(3)]
    smoothing = [None] * 25
    for field in range(25):
        tile = centre[field]
        edge = border(from_left[...], from_right[...], 2 * field + plane)
        around_x = along_lanes(tile, edge)
        around_y = tuple(
            ext[field, plane, PAD + off : last + off, :] for off in (-2, -1, 1, 2)
        )
        around_z = tuple(layer(field, plane + off) for off in (-2, -1, 1, 2))
        total_near, total_far = None, None
        for direction, around in enumerate((around_x, around_y, around_z)):
            back2, back1, ahead1, ahead2 = around
            near, far = back1 + ahead1, back2 + ahead2
            gradients[direction][field] = slope(around)
            if field <= 6 or 17 <= field <= 20:
                curves[direction][field] = (
                    (16.0 / 12.0) * near - (1.0 / 12.0) * far - (30.0 / 12.0) * tile
                )
            total_near = near if total_near is None else total_near + near
            total_far = far if total_far is None else total_far + far
        smoothing[field] = total_far - 4.0 * total_near + 18.0 * tile
    mixed_terms = {(0, 1): [], (0, 2): [], (1, 2): []}
    for slot in range(5):
        mixed_terms[0, 1].append(
            slope(
                tuple(
                    cross_x[slot, plane + 2, PAD + off : last + off, :]
                    for off in (-2, -1, 1, 2)
                )
            )
        )
        mixed_terms[0, 2].append(
            slope(
                tuple(
                    cross_x[slot, plane + 2 + off, PAD:last, :] for off in (-2, -1, 1, 2)
                )
            )
        )
        mixed_terms[1, 2].append(
            slope(tuple(cross_y[slot, plane + 2 + off] for off in (-2, -1, 1, 2)))
        )
    rates = evolve_rate(centre, gradients, curves, mixed_terms)
    for field in range(25):
        rate = rates[field] + (-DISSIPATE / 16.0) * smoothing[field]
        next_section[field, plane] = base[field, plane] + (0.5 * STEP_DT) * rate
        next_accum[field, plane] = accum[field, plane] + (STEP_DT / 3.0) * rate


def evolve_rate(centre, gradients, curves, mixed_terms):
    def second_of(chosen_slot, field_slot, axis_one, axis_two):
        if axis_one == axis_two:
            return curves[axis_one][field_slot]
        return mixed_terms[min(axis_one, axis_two), max(axis_one, axis_two)][chosen_slot]

    def metric_of(axis_one, axis_two):
        return centre[1 + PAIR_SLOT[axis_one][axis_two]]

    def traceless_of(axis_one, axis_two):
        return centre[8 + PAIR_SLOT[axis_one][axis_two]]

    def inverse_of(axis_one, axis_two):
        return (2.0 if axis_one == axis_two else 0.0) - metric_of(axis_one, axis_two)

    def advect(field_slot):
        return (
            centre[18] * gradients[0][field_slot]
            + centre[19] * gradients[1][field_slot]
            + centre[20] * gradients[2][field_slot]
        )

    conformal = centre[0]
    trace_curv = centre[7]
    lapse_field = centre[17]
    theta_field = centre[24]
    divergence = gradients[0][18] + gradients[1][19] + gradients[2][20]
    lap_conformal = curves[0][0] + curves[1][0] + curves[2][0]
    squares_a = sum(
        (traceless_of(axis_one, axis_two) ** 2 for axis_one in range(3) for axis_two in range(3))
    )

    def lapse_dd(axis_one, axis_two):
        return second_of(1, 17, axis_one, axis_two)

    ricci_table = []
    for axis_one, axis_two in PAIR_LIST:
        field_slot = 1 + PAIR_SLOT[axis_one][axis_two]
        flat_part = curves[0][field_slot] + curves[1][field_slot] + curves[2][field_slot]
        conformal_part = second_of(0, 0, axis_one, axis_two) + (
            lap_conformal if axis_one == axis_two else 0.0
        )
        ricci_table.append(
            -0.5 * flat_part
            + 0.5 * (gradients[axis_one][14 + axis_two] + gradients[axis_two][14 + axis_one])
            + conformal_part / (2.0 * conformal)
        )

    def ricci_of(axis_one, axis_two):
        return ricci_table[PAIR_SLOT[axis_one][axis_two]]

    ricci_scalar = conformal * sum(
        (
            inverse_of(axis_one, axis_two) * ricci_of(axis_one, axis_two)
            for axis_one in range(3)
            for axis_two in range(3)
        )
    )
    lapse_trace = sum(
        (
            inverse_of(axis_one, axis_two) * lapse_dd(axis_one, axis_two)
            for axis_one in range(3)
            for axis_two in range(3)
        )
    )
    rates = [None] * 25
    rates[0] = advect(0) + 2.0 / 3.0 * conformal * (lapse_field * trace_curv - divergence)
    for axis_one, axis_two in PAIR_LIST:
        field_slot = PAIR_SLOT[axis_one][axis_two]
        lie_part = sum(
            (
                metric_of(axis_one, axis_sum) * gradients[axis_two][18 + axis_sum]
                + metric_of(axis_two, axis_sum) * gradients[axis_one][18 + axis_sum]
                for axis_sum in range(3)
            )
        )
        rates[1 + field_slot] = (
            advect(1 + field_slot)
            - 2.0 * lapse_field * traceless_of(axis_one, axis_two)
            + lie_part
            - 2.0 / 3.0 * metric_of(axis_one, axis_two) * divergence
        )
    rates[7] = (
        advect(7)
        - conformal * lapse_trace
        + lapse_field * (squares_a + trace_curv * trace_curv / 3.0)
        + KAPPA_ONE * lapse_field * theta_field
    )

    def source_of(axis_one, axis_two):
        return -lapse_dd(axis_one, axis_two) + lapse_field * ricci_of(axis_one, axis_two)

    trace_part = sum(
        (
            inverse_of(axis_one, axis_two) * source_of(axis_one, axis_two)
            for axis_one in range(3)
            for axis_two in range(3)
        )
    )
    for axis_one, axis_two in PAIR_LIST:
        field_slot = PAIR_SLOT[axis_one][axis_two]
        free_part = source_of(axis_one, axis_two) - metric_of(axis_one, axis_two) * trace_part / 3.0
        product_part = sum(
            (
                traceless_of(axis_one, axis_sum) * traceless_of(axis_sum, axis_two)
                for axis_sum in range(3)
            )
        )
        lie_part = sum(
            (
                traceless_of(axis_one, axis_sum) * gradients[axis_two][18 + axis_sum]
                + traceless_of(axis_two, axis_sum) * gradients[axis_one][18 + axis_sum]
                for axis_sum in range(3)
            )
        )
        rates[8 + field_slot] = (
            advect(8 + field_slot)
            + conformal * free_part
            + lapse_field * (trace_curv * traceless_of(axis_one, axis_two) - 2.0 * product_part)
            + lie_part
            - 2.0 / 3.0 * traceless_of(axis_one, axis_two) * divergence
        )
    for axis_one in range(3):
        gauge_part = (
            -2.0
            * sum(
                (
                    traceless_of(axis_one, axis_two) * gradients[axis_two][17]
                    for axis_two in range(3)
                )
            )
            + 2.0
            * lapse_field
            * (
                -(2.0 / 3.0)
                * sum(
                    (
                        inverse_of(axis_one, axis_two) * gradients[axis_two][7]
                        for axis_two in range(3)
                    )
                )
                - 1.5
                * sum(
                    (
                        traceless_of(axis_one, axis_two) * gradients[axis_two][0]
                        for axis_two in range(3)
                    )
                )
                / conformal
            )
            + curves[0][18 + axis_one]
            + curves[1][18 + axis_one]
            + curves[2][18 + axis_one]
            + sum(
                (
                    second_of(2 + axis_two, 18 + axis_two, axis_one, axis_two)
                    for axis_two in range(3)
                )
            )
            / 3.0
            + 2.0 / 3.0 * centre[14 + axis_one] * divergence
            - sum(
                (
                    centre[14 + axis_two] * gradients[axis_two][18 + axis_one]
                    for axis_two in range(3)
                )
            )
        )
        rates[14 + axis_one] = advect(14 + axis_one) + gauge_part
        rates[18 + axis_one] = advect(18 + axis_one) + 0.75 * centre[21 + axis_one]
        rates[21 + axis_one] = (
            advect(21 + axis_one) + gauge_part - DRIVER_ETA * centre[21 + axis_one]
        )
    rates[17] = advect(17) - 2.0 * lapse_field * (trace_curv - 2.0 * theta_field)
    rates[24] = (
        advect(24)
        + 0.5 * lapse_field * (ricci_scalar + 2.0 / 3.0 * trace_curv * trace_curv - squares_a)
        - 2.0 * KAPPA_ONE * lapse_field * theta_field
    )
    return rates


AXES = ("gx", "gy", "gz")
N_GX = 4
N_GY = 4


def turned(axis, sense):
    pairs = []
    size_z = lax.axis_size("gz")
    for col in range(N_GX):
        for row in range(N_GY):
            for deep in range(size_z):
                step = sense if deep % 2 == 0 else -sense
                to_col = (col + step) % N_GX if axis == "gx" else col
                to_row = (row + step) % N_GY if axis == "gy" else row
                pairs.append(
                    ((col * N_GY + row) * size_z + deep, (to_col * N_GY + to_row) * size_z + deep)
                )
    return pairs


def place_kernel(step_y, *refs):
    own, first, second, back, slab, sems = refs[0], refs[1], refs[2], refs[3], refs[-2], refs[-1]
    sense = 1 - 2 * lax.rem(lax.axis_index("gz"), 2)
    row = lax.rem(lax.axis_index("gy") - sense * step_y + 2 * N_GY, N_GY)
    height, width = own.shape[2], own.shape[3]
    copies = []
    for number, (piece, away) in enumerate(((own, 0), (first, 1), (second, 2), (back, -1))):
        col = lax.rem(lax.axis_index("gx") - sense * away + 2 * N_GX, N_GX)
        copies.append(
            pltpu.make_async_copy(
                piece,
                slab.at[
                    :,
                    :,
                    pl.ds(pl.multiple_of(row * height, height), height),
                    pl.ds(pl.multiple_of(col * width, width), width),
                ],
                sems.at[number],
            )
        )
    for copy in copies:
        copy.start()
    for copy in copies:
        copy.wait()


def placed(slab, pieces, step_y):
    fields_count, planes, height, width = pieces[0].shape
    shape = jax.ShapeDtypeStruct((fields_count, planes, N_GY * height, N_GX * width), jnp.float32)
    args = list(pieces)
    specs = [pl.BlockSpec(memory_space=pltpu.VMEM)] * 4
    aliases = {}
    if slab is not None:
        args.append(slab)
        specs.append(pl.BlockSpec(memory_space=pl.ANY))
        aliases = {4: 0}
    return pl.pallas_call(
        lambda *refs: place_kernel(step_y, *refs),
        out_shape=shape,
        in_specs=specs,
        out_specs=pl.BlockSpec(memory_space=pl.ANY),
        scratch_shapes=[pltpu.SemaphoreType.DMA((4,))],
        input_output_aliases=aliases,
        cost_estimate=pl.CostEstimate(flops=2000000, bytes_accessed=3300000, transcendentals=0),
        compiler_params=pltpu.CompilerParams(vmem_limit_bytes=4 * 1024 * 1024),
    )(*args)


def slab_of(block):
    along_y = turned("gy", 1)
    along_x = turned("gx", 1)
    against_x = turned("gx", -1)
    slab = None
    current = block
    for step in range(4):
        following = None
        if step < 3:
            following = lax.ppermute(current, AXES, along_y)
        first = lax.ppermute(current, AXES, along_x)
        back = lax.ppermute(current, AXES, against_x)
        second = lax.ppermute(first, AXES, along_x)
        if following is not None:
            following, first, second, back = lax.optimization_barrier(
                (following, first, second, back)
            )
        slab = placed(slab, (current, first, second, back), step)
        current = following
    return slab


def ring(axis, step):
    count = lax.axis_size(axis)
    return [(source, (source + step) % count) for source in range(count)]


def sent(array, axis, step):
    return lax.ppermute(array, axis, ring(axis, step))


def vmem(count):
    return [pl.BlockSpec(memory_space=pltpu.VMEM)] * count


def shards(section, base, accum):
    flat = jax.ShapeDtypeStruct((16, 128), jnp.float32)
    strip = jax.ShapeDtypeStruct((100, 128), jnp.float32)
    small = jax.ShapeDtypeStruct((4, 128), jnp.float32)
    block = jax.ShapeDtypeStruct(section.shape, jnp.float32)
    below = sent(section, "gz", 1)
    above = sent(section, "gz", -1)
    left, right, top, bottom = pl.pallas_call(
        pack_kernel,
        out_shape=(flat, flat, strip, strip),
        in_specs=vmem(1),
        out_specs=tuple(vmem(4)),
        compiler_params=pltpu.CompilerParams(vmem_limit_bytes=4 * 1024 * 1024),
        cost_estimate=pl.CostEstimate(flops=2000000, bytes_accessed=600000, transcendentals=0),
        name="pack",
    )(section)
    from_low = sent(bottom, "gy", 1)
    from_high = sent(top, "gy", -1)
    from_left = sent(right, "gx", 1)
    from_right = sent(left, "gx", -1)
    edges, left, right = pl.pallas_call(
        edge_kernel,
        out_shape=(jax.ShapeDtypeStruct((72, 128), jnp.float32), small, small),
        in_specs=vmem(4),
        out_specs=tuple(vmem(3)),
        compiler_params=pltpu.CompilerParams(vmem_limit_bytes=2 * 1024 * 1024),
        cost_estimate=pl.CostEstimate(flops=200000, bytes_accessed=200000, transcendentals=0),
        name="edge",
    )(from_left, from_right, from_low, from_high)
    edges_below = sent(edges, "gz", 1)
    edges_above = sent(edges, "gz", -1)
    corner_left = sent(right, "gx", 1)
    corner_right = sent(left, "gx", -1)
    next_section, next_accum = pl.pallas_call(
        rate_kernel,
        out_shape=(block, block),
        in_specs=vmem(13),
        out_specs=tuple(vmem(2)),
        scratch_shapes=[
            pltpu.VMEM((29, 2, 32, 128), jnp.float32),
            pltpu.VMEM((5, 6, 32, 128), jnp.float32),
            pltpu.VMEM((5, 6, 16, 128), jnp.float32),
        ],
        compiler_params=pltpu.CompilerParams(vmem_limit_bytes=16 * 1024 * 1024),
        cost_estimate=pl.CostEstimate(flops=30000000, bytes_accessed=3000000, transcendentals=0),
        name="rate",
    )(
        section,
        below,
        above,
        from_left,
        from_right,
        from_low,
        from_high,
        edges_below,
        edges_above,
        corner_left,
        corner_right,
        base,
        accum,
    )
    return (next_section, next_accum, slab_of(next_section))


def solution(mesh):
    split = P(None, "gz", "gy", "gx")
    return jax.shard_map(
        shards,
        mesh=mesh,
        in_specs=(split, split, split),
        out_specs=(split, split, P(None, "gz", None, None)),
        check_vma=False,
    )
```

```python
import jax
import jax.numpy as jnp
from jax import lax
from jax.experimental import pallas as pl
from jax.experimental.pallas import tpu as pltpu
from jax.sharding import PartitionSpec as P


STEP_DT = 0.25
DISSIPATE = 0.1
DRIVER_ETA = 2.0
KAPPA_ONE = 0.1
PAIR_SLOT = ((0, 1, 2), (1, 3, 4), (2, 4, 5))
PAIR_LIST = ((0, 0), (0, 1), (0, 2), (1, 1), (1, 2), (2, 2))


EDGED = (0, 17, 18, 19, 20)
PAD = 8


def rolled(tile, amount):
    amount = amount % 128
    return tile if amount == 0 else pltpu.roll(tile, amount, 1)


def lanes_of(tile):
    return lax.broadcasted_iota(jnp.int32, tile.shape, 1)


def pack_kernel(section, held, left, right, top, bottom):
    fields_count, planes, rows, cols = section.shape
    low = jnp.zeros((rows, cols), jnp.float32)
    high = jnp.zeros((rows, cols), jnp.float32)
    lane_pair = lanes_of(low) // 2
    for field in range(fields_count):
        for plane in range(planes):
            number = field * planes + plane
            tile = section[field, plane]
            held[field, plane] = tile
            low = jnp.where(lane_pair == number, rolled(tile, 2 * number), low)
            high = jnp.where(lane_pair == number, rolled(tile, 2 * number + 2), high)
            top[2 * number : 2 * number + 2, :] = section[field, plane, 0:2, :]
            bottom[2 * number : 2 * number + 2, :] = section[field, plane, rows - 2 : rows, :]
    left[...] = low
    right[...] = high


def edge_kernel(from_left, from_right, from_low, from_high, edges, left, right):
    edges[0:16, :] = from_left[...]
    edges[16:32, :] = from_right[...]
    for side, rows in enumerate((from_low, from_high)):
        low = jnp.zeros((2, 128), jnp.float32)
        high = jnp.zeros((2, 128), jnp.float32)
        lane_pair = lanes_of(low) // 2
        for slot, field in enumerate(EDGED):
            for plane in range(2):
                number = slot * 2 + plane
                tile = rows[4 * field + 2 * plane : 4 * field + 2 * plane + 2, :]
                place = 32 + 20 * side + 2 * number
                edges[place : place + 2, :] = tile
                low = jnp.where(lane_pair == number, rolled(tile, 2 * number), low)
                high = jnp.where(lane_pair == number, rolled(tile, 2 * number + 2), high)
        left[2 * side : 2 * side + 2, :] = low
        right[2 * side : 2 * side + 2, :] = high


def border(from_left, from_right, number):
    return jnp.where(
        lanes_of(from_left) >= 64,
        rolled(from_left, 126 - 2 * number),
        rolled(from_right, 128 - 2 * number),
    )


def along_lanes(tile, edge):
    lane = lanes_of(tile)
    return (
        rolled(jnp.where(lane >= 126, edge, tile), 2),
        rolled(jnp.where(lane == 127, edge, tile), 1),
        rolled(jnp.where(lane == 0, edge, tile), 127),
        rolled(jnp.where(lane <= 1, edge, tile), 126),
    )


def slope(around):
    back2, back1, ahead1, ahead2 = around
    return (8.0 / 12.0) * (ahead1 - back1) - (1.0 / 12.0) * (ahead2 - back2)


TILE = 8


def rate_kernel(
    section,
    below,
    above,
    from_left,
    from_right,
    from_low,
    from_high,
    edges_below,
    edges_above,
    corner_left,
    corner_right,
    base,
    accum,
    next_section,
    next_accum,
    ext,
    side,
    cross_x,
    cross_y,
):
    fields_count, planes, rows, _ = section.shape
    last = PAD + rows

    def fill(field, carry):
        for plane in range(planes):
            ext[field, plane, PAD:last, :] = below[field, plane]
            ext[field, planes + plane, PAD:last, :] = section[field, plane]
            ext[field, 2 * planes + plane, PAD:last, :] = above[field, plane]
        return carry

    lax.fori_loop(0, fields_count, fill, 0)
    for field in range(fields_count):
        for plane in range(planes):
            number = field * planes + plane
            side[field, plane] = border(from_left[...], from_right[...], number)
            place = 2 * number
            ext[field, plane + 2, PAD - 2 : PAD, :] = from_low[place : place + 2, :]
            ext[field, plane + 2, last : last + 2, :] = from_high[place : place + 2, :]
    for slot, field in enumerate(EDGED):
        for layer in range(6):
            if layer in (2, 3):
                edge = side[field, layer - 2]
                for number, place in enumerate((PAD - 2, last)):
                    strip = border(
                        corner_left[2 * number : 2 * number + 2, :],
                        corner_right[2 * number : 2 * number + 2, :],
                        2 * slot + layer - 2,
                    )
                    cross_x[slot, layer, place : place + 2, :] = slope(
                        along_lanes(ext[field, layer, place : place + 2, :], strip)
                    )
            else:
                source, local = (edges_below, layer) if layer < 2 else (edges_above, layer - 4)
                edge = border(source[0:16, :], source[16:32, :], 2 * field + local)
                place = 4 * slot + 2 * local
                ext[field, layer, PAD - 2 : PAD, :] = source[32 + place : 34 + place, :]
                ext[field, layer, last : last + 2, :] = source[52 + place : 54 + place, :]
            cross_x[slot, layer, PAD:last, :] = slope(
                along_lanes(ext[field, layer, PAD:last, :], edge)
            )

    def tilt(number, carry):
        slot = number // 6
        layer = number % 6
        field = jnp.where(slot == 0, 0, slot + 16)
        cross_y[slot, layer] = slope(
            tuple(ext[field, layer, PAD + off : last + off, :] for off in (-2, -1, 1, 2))
        )
        return carry

    lax.fori_loop(0, 30, tilt, 0)

    def tile_rates(number, carry):
        write_rates(
            number, side, base, accum, next_section, next_accum, ext, cross_x, cross_y
        )
        return carry

    lax.fori_loop(0, planes * rows // TILE, tile_rates, 0)


def write_rates(number, side, base, accum, next_section, next_accum, ext, cross_x, cross_y):
    parts = 16 // TILE
    plane = number // parts
    start = 0 if parts == 1 else pl.multiple_of((number % parts) * TILE, TILE)

    def span(begin):
        if parts == 1:
            return slice(begin, begin + TILE)
        return pl.ds(start + begin, TILE)

    centre = [ext[field, plane + 2, span(PAD), :] for field in range(25)]
    gradients = [[None] * 25 for _ in range(3)]
    curves = [[None] * 25 for _ in range(3)]
    smoothing = [None] * 25
    for field in range(25):
        tile = centre[field]
        around_x = along_lanes(tile, side[field, plane, span(0), :])
        around_y = tuple(ext[field, plane + 2, span(PAD + off), :] for off in (-2, -1, 1, 2))
        around_z = tuple(ext[field, plane + 2 + off, span(PAD), :] for off in (-2, -1, 1, 2))
        total_near, total_far = None, None
        for direction, around in enumerate((around_x, around_y, around_z)):
            back2, back1, ahead1, ahead2 = around
            near, far = back1 + ahead1, back2 + ahead2
            gradients[direction][field] = slope(around)
            if field <= 6 or 17 <= field <= 20:
                curves[direction][field] = (
                    (16.0 / 12.0) * near - (1.0 / 12.0) * far - (30.0 / 12.0) * tile
                )
            total_near = near if total_near is None else total_near + near
            total_far = far if total_far is None else total_far + far
        smoothing[field] = total_far - 4.0 * total_near + 18.0 * tile
    mixed_terms = {(0, 1): [], (0, 2): [], (1, 2): []}
    offsets = (-2, -1, 1, 2)
    for slot in range(5):
        mixed_terms[0, 1].append(
            slope(tuple(cross_x[slot, plane + 2, span(PAD + off), :] for off in offsets))
        )
        mixed_terms[0, 2].append(
            slope(tuple(cross_x[slot, plane + 2 + off, span(PAD), :] for off in offsets))
        )
        mixed_terms[1, 2].append(
            slope(tuple(cross_y[slot, plane + 2 + off, span(0), :] for off in offsets))
        )
    rates = evolve_rate(centre, gradients, curves, mixed_terms)
    for field in range(25):
        rate = rates[field] + (-DISSIPATE / 16.0) * smoothing[field]
        next_section[field, plane, span(0), :] = (
            base[field, plane, span(0), :] + (0.5 * STEP_DT) * rate
        )
        next_accum[field, plane, span(0), :] = (
            accum[field, plane, span(0), :] + (STEP_DT / 3.0) * rate
        )


def evolve_rate(centre, gradients, curves, mixed_terms):
    def second_of(chosen_slot, field_slot, axis_one, axis_two):
        if axis_one == axis_two:
            return curves[axis_one][field_slot]
        return mixed_terms[min(axis_one, axis_two), max(axis_one, axis_two)][chosen_slot]

    def metric_of(axis_one, axis_two):
        return centre[1 + PAIR_SLOT[axis_one][axis_two]]

    def traceless_of(axis_one, axis_two):
        return centre[8 + PAIR_SLOT[axis_one][axis_two]]

    def inverse_of(axis_one, axis_two):
        return (2.0 if axis_one == axis_two else 0.0) - metric_of(axis_one, axis_two)

    def advect(field_slot):
        return (
            centre[18] * gradients[0][field_slot]
            + centre[19] * gradients[1][field_slot]
            + centre[20] * gradients[2][field_slot]
        )

    conformal = centre[0]
    trace_curv = centre[7]
    lapse_field = centre[17]
    theta_field = centre[24]
    divergence = gradients[0][18] + gradients[1][19] + gradients[2][20]
    lap_conformal = curves[0][0] + curves[1][0] + curves[2][0]
    squares_a = sum(
        (traceless_of(axis_one, axis_two) ** 2 for axis_one in range(3) for axis_two in range(3))
    )

    def lapse_dd(axis_one, axis_two):
        return second_of(1, 17, axis_one, axis_two)

    ricci_table = []
    for axis_one, axis_two in PAIR_LIST:
        field_slot = 1 + PAIR_SLOT[axis_one][axis_two]
        flat_part = curves[0][field_slot] + curves[1][field_slot] + curves[2][field_slot]
        conformal_part = second_of(0, 0, axis_one, axis_two) + (
            lap_conformal if axis_one == axis_two else 0.0
        )
        ricci_table.append(
            -0.5 * flat_part
            + 0.5 * (gradients[axis_one][14 + axis_two] + gradients[axis_two][14 + axis_one])
            + conformal_part / (2.0 * conformal)
        )

    def ricci_of(axis_one, axis_two):
        return ricci_table[PAIR_SLOT[axis_one][axis_two]]

    ricci_scalar = conformal * sum(
        (
            inverse_of(axis_one, axis_two) * ricci_of(axis_one, axis_two)
            for axis_one in range(3)
            for axis_two in range(3)
        )
    )
    lapse_trace = sum(
        (
            inverse_of(axis_one, axis_two) * lapse_dd(axis_one, axis_two)
            for axis_one in range(3)
            for axis_two in range(3)
        )
    )
    rates = [None] * 25
    rates[0] = advect(0) + 2.0 / 3.0 * conformal * (lapse_field * trace_curv - divergence)
    for axis_one, axis_two in PAIR_LIST:
        field_slot = PAIR_SLOT[axis_one][axis_two]
        lie_part = sum(
            (
                metric_of(axis_one, axis_sum) * gradients[axis_two][18 + axis_sum]
                + metric_of(axis_two, axis_sum) * gradients[axis_one][18 + axis_sum]
                for axis_sum in range(3)
            )
        )
        rates[1 + field_slot] = (
            advect(1 + field_slot)
            - 2.0 * lapse_field * traceless_of(axis_one, axis_two)
            + lie_part
            - 2.0 / 3.0 * metric_of(axis_one, axis_two) * divergence
        )
    rates[7] = (
        advect(7)
        - conformal * lapse_trace
        + lapse_field * (squares_a + trace_curv * trace_curv / 3.0)
        + KAPPA_ONE * lapse_field * theta_field
    )

    def source_of(axis_one, axis_two):
        return -lapse_dd(axis_one, axis_two) + lapse_field * ricci_of(axis_one, axis_two)

    trace_part = sum(
        (
            inverse_of(axis_one, axis_two) * source_of(axis_one, axis_two)
            for axis_one in range(3)
            for axis_two in range(3)
        )
    )
    for axis_one, axis_two in PAIR_LIST:
        field_slot = PAIR_SLOT[axis_one][axis_two]
        free_part = source_of(axis_one, axis_two) - metric_of(axis_one, axis_two) * trace_part / 3.0
        product_part = sum(
            (
                traceless_of(axis_one, axis_sum) * traceless_of(axis_sum, axis_two)
                for axis_sum in range(3)
            )
        )
        lie_part = sum(
            (
                traceless_of(axis_one, axis_sum) * gradients[axis_two][18 + axis_sum]
                + traceless_of(axis_two, axis_sum) * gradients[axis_one][18 + axis_sum]
                for axis_sum in range(3)
            )
        )
        rates[8 + field_slot] = (
            advect(8 + field_slot)
            + conformal * free_part
            + lapse_field * (trace_curv * traceless_of(axis_one, axis_two) - 2.0 * product_part)
            + lie_part
            - 2.0 / 3.0 * traceless_of(axis_one, axis_two) * divergence
        )
    for axis_one in range(3):
        gauge_part = (
            -2.0
            * sum(
                (
                    traceless_of(axis_one, axis_two) * gradients[axis_two][17]
                    for axis_two in range(3)
                )
            )
            + 2.0
            * lapse_field
            * (
                -(2.0 / 3.0)
                * sum(
                    (
                        inverse_of(axis_one, axis_two) * gradients[axis_two][7]
                        for axis_two in range(3)
                    )
                )
                - 1.5
                * sum(
                    (
                        traceless_of(axis_one, axis_two) * gradients[axis_two][0]
                        for axis_two in range(3)
                    )
                )
                / conformal
            )
            + curves[0][18 + axis_one]
            + curves[1][18 + axis_one]
            + curves[2][18 + axis_one]
            + sum(
                (
                    second_of(2 + axis_two, 18 + axis_two, axis_one, axis_two)
                    for axis_two in range(3)
                )
            )
            / 3.0
            + 2.0 / 3.0 * centre[14 + axis_one] * divergence
            - sum(
                (
                    centre[14 + axis_two] * gradients[axis_two][18 + axis_one]
                    for axis_two in range(3)
                )
            )
        )
        rates[14 + axis_one] = advect(14 + axis_one) + gauge_part
        rates[18 + axis_one] = advect(18 + axis_one) + 0.75 * centre[21 + axis_one]
        rates[21 + axis_one] = (
            advect(21 + axis_one) + gauge_part - DRIVER_ETA * centre[21 + axis_one]
        )
    rates[17] = advect(17) - 2.0 * lapse_field * (trace_curv - 2.0 * theta_field)
    rates[24] = (
        advect(24)
        + 0.5 * lapse_field * (ricci_scalar + 2.0 / 3.0 * trace_curv * trace_curv - squares_a)
        - 2.0 * KAPPA_ONE * lapse_field * theta_field
    )
    return rates


AXES = ("gx", "gy", "gz")
N_GX = 4
N_GY = 4


def turned(axis, sense):
    pairs = []
    size_z = lax.axis_size("gz")
    for col in range(N_GX):
        for row in range(N_GY):
            for deep in range(size_z):
                step = sense if deep % 2 == 0 else -sense
                to_col = (col + step) % N_GX if axis == "gx" else col
                to_row = (row + step) % N_GY if axis == "gy" else row
                pairs.append(
                    ((col * N_GY + row) * size_z + deep, (to_col * N_GY + to_row) * size_z + deep)
                )
    return pairs


def place_kernel(step_y, *refs):
    own, first, second, back, slab, sems = refs[0], refs[1], refs[2], refs[3], refs[-2], refs[-1]
    sense = 1 - 2 * lax.rem(lax.axis_index("gz"), 2)
    row = lax.rem(lax.axis_index("gy") - sense * step_y + 2 * N_GY, N_GY)
    height, width = own.shape[2], own.shape[3]
    copies = []
    for number, (piece, away) in enumerate(((own, 0), (first, 1), (second, 2), (back, -1))):
        col = lax.rem(lax.axis_index("gx") - sense * away + 2 * N_GX, N_GX)
        copies.append(
            pltpu.make_async_copy(
                piece,
                slab.at[
                    :,
                    :,
                    pl.ds(pl.multiple_of(row * height, height), height),
                    pl.ds(pl.multiple_of(col * width, width), width),
                ],
                sems.at[number],
            )
        )
    for copy in copies:
        copy.start()
    for copy in copies:
        copy.wait()


def placed(slab, pieces, step_y):
    fields_count, planes, height, width = pieces[0].shape
    shape = jax.ShapeDtypeStruct((fields_count, planes, N_GY * height, N_GX * width), jnp.float32)
    args = list(pieces)
    specs = [pl.BlockSpec(memory_space=pltpu.VMEM)] * 4
    aliases = {}
    if slab is not None:
        args.append(slab)
        specs.append(pl.BlockSpec(memory_space=pl.ANY))
        aliases = {4: 0}
    return pl.pallas_call(
        lambda *refs: place_kernel(step_y, *refs),
        out_shape=shape,
        in_specs=specs,
        out_specs=pl.BlockSpec(memory_space=pl.ANY),
        scratch_shapes=[pltpu.SemaphoreType.DMA((4,))],
        input_output_aliases=aliases,
        cost_estimate=pl.CostEstimate(flops=2000000, bytes_accessed=3300000, transcendentals=0),
        compiler_params=pltpu.CompilerParams(vmem_limit_bytes=4 * 1024 * 1024),
    )(*args)


def slab_of(block):
    along_y = turned("gy", 1)
    along_x = turned("gx", 1)
    against_x = turned("gx", -1)
    slab = None
    current = block
    for step in range(4):
        following = None
        if step < 3:
            following = lax.ppermute(current, AXES, along_y)
        first = lax.ppermute(current, AXES, along_x)
        back = lax.ppermute(current, AXES, against_x)
        second = lax.ppermute(first, AXES, along_x)
        if following is not None:
            following, first, second, back = lax.optimization_barrier(
                (following, first, second, back)
            )
        slab = placed(slab, (current, first, second, back), step)
        current = following
    return slab


def ring(axis, step):
    count = lax.axis_size(axis)
    return [(source, (source + step) % count) for source in range(count)]


def sent(array, axis, step):
    return lax.ppermute(array, axis, ring(axis, step))


def vmem(count):
    return [pl.BlockSpec(memory_space=pltpu.VMEM)] * count


def shards(section, base, accum):
    flat = jax.ShapeDtypeStruct((16, 128), jnp.float32)
    strip = jax.ShapeDtypeStruct((100, 128), jnp.float32)
    small = jax.ShapeDtypeStruct((4, 128), jnp.float32)
    block = jax.ShapeDtypeStruct(section.shape, jnp.float32)
    below = sent(section, "gz", 1)
    above = sent(section, "gz", -1)
    held, left, right, top, bottom = pl.pallas_call(
        pack_kernel,
        out_shape=(block, flat, flat, strip, strip),
        in_specs=vmem(1),
        out_specs=tuple(vmem(5)),
        compiler_params=pltpu.CompilerParams(vmem_limit_bytes=4 * 1024 * 1024),
        cost_estimate=pl.CostEstimate(flops=2000000, bytes_accessed=600000, transcendentals=0),
        name="pack",
    )(section)
    from_low = sent(bottom, "gy", 1)
    from_high = sent(top, "gy", -1)
    from_left = sent(right, "gx", 1)
    from_right = sent(left, "gx", -1)
    edges, left, right = pl.pallas_call(
        edge_kernel,
        out_shape=(jax.ShapeDtypeStruct((72, 128), jnp.float32), small, small),
        in_specs=vmem(4),
        out_specs=tuple(vmem(3)),
        compiler_params=pltpu.CompilerParams(vmem_limit_bytes=2 * 1024 * 1024),
        cost_estimate=pl.CostEstimate(flops=200000, bytes_accessed=200000, transcendentals=0),
        name="edge",
    )(from_left, from_right, from_low, from_high)
    edges_below = sent(edges, "gz", 1)
    edges_above = sent(edges, "gz", -1)
    corner_left = sent(right, "gx", 1)
    corner_right = sent(left, "gx", -1)
    next_section, next_accum = pl.pallas_call(
        rate_kernel,
        out_shape=(block, block),
        in_specs=vmem(13),
        out_specs=tuple(vmem(2)),
        scratch_shapes=[
            pltpu.VMEM((25, 6, 32, 128), jnp.float32),
            pltpu.VMEM((25, 2, 16, 128), jnp.float32),
            pltpu.VMEM((5, 6, 32, 128), jnp.float32),
            pltpu.VMEM((5, 6, 16, 128), jnp.float32),
        ],
        compiler_params=pltpu.CompilerParams(vmem_limit_bytes=16 * 1024 * 1024),
        cost_estimate=pl.CostEstimate(flops=30000000, bytes_accessed=3000000, transcendentals=0),
        name="rate",
    )(
        held,
        below,
        above,
        from_left,
        from_right,
        from_low,
        from_high,
        edges_below,
        edges_above,
        corner_left,
        corner_right,
        base,
        accum,
    )
    return (next_section, next_accum, slab_of(next_section))


def solution(mesh):
    split = P(None, "gz", "gy", "gx")
    return jax.shard_map(
        shards,
        mesh=mesh,
        in_specs=(split, split, split),
        out_specs=(split, split, P(None, "gz", None, None)),
        check_vma=False,
    )
```

```python
import jax
import jax.numpy as jnp
from jax import lax
from jax.experimental import pallas as pl
from jax.experimental.pallas import tpu as pltpu
from jax.sharding import PartitionSpec as P


STEP_DT = 0.25
DISSIPATE = 0.1
DRIVER_ETA = 2.0
KAPPA_ONE = 0.1
PAIR_SLOT = ((0, 1, 2), (1, 3, 4), (2, 4, 5))
PAIR_LIST = ((0, 0), (0, 1), (0, 2), (1, 1), (1, 2), (2, 2))


EDGED = (0, 17, 18, 19, 20)
PAD = 8


def rolled(tile, amount):
    amount = amount % 128
    return tile if amount == 0 else pltpu.roll(tile, amount, 1)


def lanes_of(tile):
    return lax.broadcasted_iota(jnp.int32, tile.shape, 1)


def pack_kernel(section, held, left, right, top, bottom):
    fields_count, planes, rows, cols = section.shape
    low = jnp.zeros((rows, cols), jnp.float32)
    high = jnp.zeros((rows, cols), jnp.float32)
    lane_pair = lanes_of(low) // 2
    for field in range(fields_count):
        for plane in range(planes):
            number = field * planes + plane
            tile = section[field, plane]
            held[field, plane] = tile
            low = jnp.where(lane_pair == number, rolled(tile, 2 * number), low)
            high = jnp.where(lane_pair == number, rolled(tile, 2 * number + 2), high)
            top[2 * number : 2 * number + 2, :] = section[field, plane, 0:2, :]
            bottom[2 * number : 2 * number + 2, :] = section[field, plane, rows - 2 : rows, :]
    left[...] = low
    right[...] = high


def edge_kernel(from_left, from_right, from_low, from_high, edges, left, right):
    edges[0:16, :] = from_left[...]
    edges[16:32, :] = from_right[...]
    for side, rows in enumerate((from_low, from_high)):
        low = jnp.zeros((2, 128), jnp.float32)
        high = jnp.zeros((2, 128), jnp.float32)
        lane_pair = lanes_of(low) // 2
        for slot, field in enumerate(EDGED):
            for plane in range(2):
                number = slot * 2 + plane
                tile = rows[4 * field + 2 * plane : 4 * field + 2 * plane + 2, :]
                place = 32 + 20 * side + 2 * number
                edges[place : place + 2, :] = tile
                low = jnp.where(lane_pair == number, rolled(tile, 2 * number), low)
                high = jnp.where(lane_pair == number, rolled(tile, 2 * number + 2), high)
        left[2 * side : 2 * side + 2, :] = low
        right[2 * side : 2 * side + 2, :] = high


def border(from_left, from_right, number):
    return jnp.where(
        lanes_of(from_left) >= 64,
        rolled(from_left, 126 - 2 * number),
        rolled(from_right, 128 - 2 * number),
    )


def along_lanes(tile, edge):
    lane = lanes_of(tile)
    return (
        rolled(jnp.where(lane >= 126, edge, tile), 2),
        rolled(jnp.where(lane == 127, edge, tile), 1),
        rolled(jnp.where(lane == 0, edge, tile), 127),
        rolled(jnp.where(lane <= 1, edge, tile), 126),
    )


def slope(around):
    back2, back1, ahead1, ahead2 = around
    return (8.0 / 12.0) * (ahead1 - back1) - (1.0 / 12.0) * (ahead2 - back2)


TILE = 8


def rate_kernel(
    section,
    below,
    above,
    from_left,
    from_right,
    from_low,
    from_high,
    edges_below,
    edges_above,
    corner_left,
    corner_right,
    base,
    next_section,
    held,
    rates,
    ext,
    side,
    cross_x,
    cross_y,
):
    fields_count, planes, rows, _ = section.shape
    last = PAD + rows

    def fill(field, carry):
        for plane in range(planes):
            ext[field, plane, PAD:last, :] = below[field, plane]
            ext[field, planes + plane, PAD:last, :] = section[field, plane]
            ext[field, 2 * planes + plane, PAD:last, :] = above[field, plane]
        return carry

    lax.fori_loop(0, fields_count, fill, 0)
    for field in range(fields_count):
        for plane in range(planes):
            number = field * planes + plane
            side[field, plane] = border(from_left[...], from_right[...], number)
            place = 2 * number
            ext[field, plane + 2, PAD - 2 : PAD, :] = from_low[place : place + 2, :]
            ext[field, plane + 2, last : last + 2, :] = from_high[place : place + 2, :]
    for slot, field in enumerate(EDGED):
        for layer in range(6):
            if layer in (2, 3):
                edge = side[field, layer - 2]
                for number, place in enumerate((PAD - 2, last)):
                    strip = border(
                        corner_left[2 * number : 2 * number + 2, :],
                        corner_right[2 * number : 2 * number + 2, :],
                        2 * slot + layer - 2,
                    )
                    cross_x[slot, layer, place : place + 2, :] = slope(
                        along_lanes(ext[field, layer, place : place + 2, :], strip)
                    )
            else:
                source, local = (edges_below, layer) if layer < 2 else (edges_above, layer - 4)
                edge = border(source[0:16, :], source[16:32, :], 2 * field + local)
                place = 4 * slot + 2 * local
                ext[field, layer, PAD - 2 : PAD, :] = source[32 + place : 34 + place, :]
                ext[field, layer, last : last + 2, :] = source[52 + place : 54 + place, :]
            cross_x[slot, layer, PAD:last, :] = slope(
                along_lanes(ext[field, layer, PAD:last, :], edge)
            )

    def tilt(number, carry):
        slot = number // 6
        layer = number % 6
        field = jnp.where(slot == 0, 0, slot + 16)
        cross_y[slot, layer] = slope(
            tuple(ext[field, layer, PAD + off : last + off, :] for off in (-2, -1, 1, 2))
        )
        return carry

    lax.fori_loop(0, 30, tilt, 0)

    def tile_rates(number, carry):
        write_rates(number, side, base, next_section, held, rates, ext, cross_x, cross_y)
        return carry

    lax.fori_loop(0, planes * rows // TILE, tile_rates, 0)


def write_rates(number, side, base, next_section, held, rates_out, ext, cross_x, cross_y):
    parts = 16 // TILE
    plane = number // parts
    start = 0 if parts == 1 else pl.multiple_of((number % parts) * TILE, TILE)

    def span(begin):
        if parts == 1:
            return slice(begin, begin + TILE)
        return pl.ds(start + begin, TILE)

    centre = [ext[field, plane + 2, span(PAD), :] for field in range(25)]
    gradients = [[None] * 25 for _ in range(3)]
    curves = [[None] * 25 for _ in range(3)]
    smoothing = [None] * 25
    for field in range(25):
        tile = centre[field]
        around_x = along_lanes(tile, side[field, plane, span(0), :])
        around_y = tuple(ext[field, plane + 2, span(PAD + off), :] for off in (-2, -1, 1, 2))
        around_z = tuple(ext[field, plane + 2 + off, span(PAD), :] for off in (-2, -1, 1, 2))
        total_near, total_far = None, None
        for direction, around in enumerate((around_x, around_y, around_z)):
            back2, back1, ahead1, ahead2 = around
            near, far = back1 + ahead1, back2 + ahead2
            gradients[direction][field] = slope(around)
            if field <= 6 or 17 <= field <= 20:
                curves[direction][field] = (
                    (16.0 / 12.0) * near - (1.0 / 12.0) * far - (30.0 / 12.0) * tile
                )
            total_near = near if total_near is None else total_near + near
            total_far = far if total_far is None else total_far + far
        smoothing[field] = total_far - 4.0 * total_near + 18.0 * tile
    mixed_terms = {(0, 1): [], (0, 2): [], (1, 2): []}
    offsets = (-2, -1, 1, 2)
    for slot in range(5):
        mixed_terms[0, 1].append(
            slope(tuple(cross_x[slot, plane + 2, span(PAD + off), :] for off in offsets))
        )
        mixed_terms[0, 2].append(
            slope(tuple(cross_x[slot, plane + 2 + off, span(PAD), :] for off in offsets))
        )
        mixed_terms[1, 2].append(
            slope(tuple(cross_y[slot, plane + 2 + off, span(0), :] for off in offsets))
        )
    rates = evolve_rate(centre, gradients, curves, mixed_terms)
    for field in range(25):
        rate = rates[field] + (-DISSIPATE / 16.0) * smoothing[field]
        result = base[field, plane, span(0), :] + (0.5 * STEP_DT) * rate
        next_section[field, plane, span(0), :] = result
        held[field, plane, span(0), :] = result
        rates_out[field, plane, span(0), :] = rate


def tally_kernel(accum, rates, next_accum):
    next_accum[...] = accum[...] + (STEP_DT / 3.0) * rates[...]


def evolve_rate(centre, gradients, curves, mixed_terms):
    def second_of(chosen_slot, field_slot, axis_one, axis_two):
        if axis_one == axis_two:
            return curves[axis_one][field_slot]
        return mixed_terms[min(axis_one, axis_two), max(axis_one, axis_two)][chosen_slot]

    def metric_of(axis_one, axis_two):
        return centre[1 + PAIR_SLOT[axis_one][axis_two]]

    def traceless_of(axis_one, axis_two):
        return centre[8 + PAIR_SLOT[axis_one][axis_two]]

    def inverse_of(axis_one, axis_two):
        return (2.0 if axis_one == axis_two else 0.0) - metric_of(axis_one, axis_two)

    def advect(field_slot):
        return (
            centre[18] * gradients[0][field_slot]
            + centre[19] * gradients[1][field_slot]
            + centre[20] * gradients[2][field_slot]
        )

    conformal = centre[0]
    trace_curv = centre[7]
    lapse_field = centre[17]
    theta_field = centre[24]
    divergence = gradients[0][18] + gradients[1][19] + gradients[2][20]
    lap_conformal = curves[0][0] + curves[1][0] + curves[2][0]
    squares_a = sum(
        (traceless_of(axis_one, axis_two) ** 2 for axis_one in range(3) for axis_two in range(3))
    )

    def lapse_dd(axis_one, axis_two):
        return second_of(1, 17, axis_one, axis_two)

    ricci_table = []
    for axis_one, axis_two in PAIR_LIST:
        field_slot = 1 + PAIR_SLOT[axis_one][axis_two]
        flat_part = curves[0][field_slot] + curves[1][field_slot] + curves[2][field_slot]
        conformal_part = second_of(0, 0, axis_one, axis_two) + (
            lap_conformal if axis_one == axis_two else 0.0
        )
        ricci_table.append(
            -0.5 * flat_part
            + 0.5 * (gradients[axis_one][14 + axis_two] + gradients[axis_two][14 + axis_one])
            + conformal_part / (2.0 * conformal)
        )

    def ricci_of(axis_one, axis_two):
        return ricci_table[PAIR_SLOT[axis_one][axis_two]]

    ricci_scalar = conformal * sum(
        (
            inverse_of(axis_one, axis_two) * ricci_of(axis_one, axis_two)
            for axis_one in range(3)
            for axis_two in range(3)
        )
    )
    lapse_trace = sum(
        (
            inverse_of(axis_one, axis_two) * lapse_dd(axis_one, axis_two)
            for axis_one in range(3)
            for axis_two in range(3)
        )
    )
    rates = [None] * 25
    rates[0] = advect(0) + 2.0 / 3.0 * conformal * (lapse_field * trace_curv - divergence)
    for axis_one, axis_two in PAIR_LIST:
        field_slot = PAIR_SLOT[axis_one][axis_two]
        lie_part = sum(
            (
                metric_of(axis_one, axis_sum) * gradients[axis_two][18 + axis_sum]
                + metric_of(axis_two, axis_sum) * gradients[axis_one][18 + axis_sum]
                for axis_sum in range(3)
            )
        )
        rates[1 + field_slot] = (
            advect(1 + field_slot)
            - 2.0 * lapse_field * traceless_of(axis_one, axis_two)
            + lie_part
            - 2.0 / 3.0 * metric_of(axis_one, axis_two) * divergence
        )
    rates[7] = (
        advect(7)
        - conformal * lapse_trace
        + lapse_field * (squares_a + trace_curv * trace_curv / 3.0)
        + KAPPA_ONE * lapse_field * theta_field
    )

    def source_of(axis_one, axis_two):
        return -lapse_dd(axis_one, axis_two) + lapse_field * ricci_of(axis_one, axis_two)

    trace_part = sum(
        (
            inverse_of(axis_one, axis_two) * source_of(axis_one, axis_two)
            for axis_one in range(3)
            for axis_two in range(3)
        )
    )
    for axis_one, axis_two in PAIR_LIST:
        field_slot = PAIR_SLOT[axis_one][axis_two]
        free_part = source_of(axis_one, axis_two) - metric_of(axis_one, axis_two) * trace_part / 3.0
        product_part = sum(
            (
                traceless_of(axis_one, axis_sum) * traceless_of(axis_sum, axis_two)
                for axis_sum in range(3)
            )
        )
        lie_part = sum(
            (
                traceless_of(axis_one, axis_sum) * gradients[axis_two][18 + axis_sum]
                + traceless_of(axis_two, axis_sum) * gradients[axis_one][18 + axis_sum]
                for axis_sum in range(3)
            )
        )
        rates[8 + field_slot] = (
            advect(8 + field_slot)
            + conformal * free_part
            + lapse_field * (trace_curv * traceless_of(axis_one, axis_two) - 2.0 * product_part)
            + lie_part
            - 2.0 / 3.0 * traceless_of(axis_one, axis_two) * divergence
        )
    for axis_one in range(3):
        gauge_part = (
            -2.0
            * sum(
                (
                    traceless_of(axis_one, axis_two) * gradients[axis_two][17]
                    for axis_two in range(3)
                )
            )
            + 2.0
            * lapse_field
            * (
                -(2.0 / 3.0)
                * sum(
                    (
                        inverse_of(axis_one, axis_two) * gradients[axis_two][7]
                        for axis_two in range(3)
                    )
                )
                - 1.5
                * sum(
                    (
                        traceless_of(axis_one, axis_two) * gradients[axis_two][0]
                        for axis_two in range(3)
                    )
                )
                / conformal
            )
            + curves[0][18 + axis_one]
            + curves[1][18 + axis_one]
            + curves[2][18 + axis_one]
            + sum(
                (
                    second_of(2 + axis_two, 18 + axis_two, axis_one, axis_two)
                    for axis_two in range(3)
                )
            )
            / 3.0
            + 2.0 / 3.0 * centre[14 + axis_one] * divergence
            - sum(
                (
                    centre[14 + axis_two] * gradients[axis_two][18 + axis_one]
                    for axis_two in range(3)
                )
            )
        )
        rates[14 + axis_one] = advect(14 + axis_one) + gauge_part
        rates[18 + axis_one] = advect(18 + axis_one) + 0.75 * centre[21 + axis_one]
        rates[21 + axis_one] = (
            advect(21 + axis_one) + gauge_part - DRIVER_ETA * centre[21 + axis_one]
        )
    rates[17] = advect(17) - 2.0 * lapse_field * (trace_curv - 2.0 * theta_field)
    rates[24] = (
        advect(24)
        + 0.5 * lapse_field * (ricci_scalar + 2.0 / 3.0 * trace_curv * trace_curv - squares_a)
        - 2.0 * KAPPA_ONE * lapse_field * theta_field
    )
    return rates


AXES = ("gx", "gy", "gz")
N_GX = 4
N_GY = 4


def turned(axis, sense):
    pairs = []
    size_z = lax.axis_size("gz")
    for col in range(N_GX):
        for row in range(N_GY):
            for deep in range(size_z):
                step = sense if deep % 2 == 0 else -sense
                to_col = (col + step) % N_GX if axis == "gx" else col
                to_row = (row + step) % N_GY if axis == "gy" else row
                pairs.append(
                    ((col * N_GY + row) * size_z + deep, (to_col * N_GY + to_row) * size_z + deep)
                )
    return pairs


def place_kernel(step_y, *refs):
    own, first, second, back, slab, sems = refs[0], refs[1], refs[2], refs[3], refs[-2], refs[-1]
    sense = 1 - 2 * lax.rem(lax.axis_index("gz"), 2)
    row = lax.rem(lax.axis_index("gy") - sense * step_y + 2 * N_GY, N_GY)
    height, width = own.shape[2], own.shape[3]
    copies = []
    for number, (piece, away) in enumerate(((own, 0), (first, 1), (second, 2), (back, -1))):
        col = lax.rem(lax.axis_index("gx") - sense * away + 2 * N_GX, N_GX)
        copies.append(
            pltpu.make_async_copy(
                piece,
                slab.at[
                    :,
                    :,
                    pl.ds(pl.multiple_of(row * height, height), height),
                    pl.ds(pl.multiple_of(col * width, width), width),
                ],
                sems.at[number],
            )
        )
    for copy in copies:
        copy.start()
    for copy in copies:
        copy.wait()


def placed(slab, pieces, step_y):
    fields_count, planes, height, width = pieces[0].shape
    shape = jax.ShapeDtypeStruct((fields_count, planes, N_GY * height, N_GX * width), jnp.float32)
    args = list(pieces)
    specs = [pl.BlockSpec(memory_space=pltpu.VMEM)] * 4
    aliases = {}
    if slab is not None:
        args.append(slab)
        specs.append(pl.BlockSpec(memory_space=pl.ANY))
        aliases = {4: 0}
    return pl.pallas_call(
        lambda *refs: place_kernel(step_y, *refs),
        out_shape=shape,
        in_specs=specs,
        out_specs=pl.BlockSpec(memory_space=pl.ANY),
        scratch_shapes=[pltpu.SemaphoreType.DMA((4,))],
        input_output_aliases=aliases,
        cost_estimate=pl.CostEstimate(flops=2000000, bytes_accessed=3300000, transcendentals=0),
        compiler_params=pltpu.CompilerParams(vmem_limit_bytes=4 * 1024 * 1024),
    )(*args)


def slab_of(block):
    along_y = turned("gy", 1)
    along_x = turned("gx", 1)
    against_x = turned("gx", -1)
    slab = None
    current = block
    for step in range(4):
        following = None
        if step < 3:
            following = lax.ppermute(current, AXES, along_y)
        first = lax.ppermute(current, AXES, along_x)
        back = lax.ppermute(current, AXES, against_x)
        second = lax.ppermute(first, AXES, along_x)
        if following is not None:
            following, first, second, back = lax.optimization_barrier(
                (following, first, second, back)
            )
        slab = placed(slab, (current, first, second, back), step)
        current = following
    return slab


def ring(axis, step):
    count = lax.axis_size(axis)
    return [(source, (source + step) % count) for source in range(count)]


def sent(array, axis, step):
    return lax.ppermute(array, axis, ring(axis, step))


def vmem(count):
    return [pl.BlockSpec(memory_space=pltpu.VMEM)] * count


def shards(section, base, accum):
    flat = jax.ShapeDtypeStruct((16, 128), jnp.float32)
    strip = jax.ShapeDtypeStruct((100, 128), jnp.float32)
    small = jax.ShapeDtypeStruct((4, 128), jnp.float32)
    block = jax.ShapeDtypeStruct(section.shape, jnp.float32)
    below = sent(section, "gz", 1)
    above = sent(section, "gz", -1)
    held, left, right, top, bottom = pl.pallas_call(
        pack_kernel,
        out_shape=(block, flat, flat, strip, strip),
        in_specs=vmem(1),
        out_specs=tuple(vmem(5)),
        compiler_params=pltpu.CompilerParams(vmem_limit_bytes=4 * 1024 * 1024),
        cost_estimate=pl.CostEstimate(flops=2000000, bytes_accessed=600000, transcendentals=0),
        name="pack",
    )(section)
    from_low = sent(bottom, "gy", 1)
    from_high = sent(top, "gy", -1)
    from_left = sent(right, "gx", 1)
    from_right = sent(left, "gx", -1)
    edges, left, right = pl.pallas_call(
        edge_kernel,
        out_shape=(jax.ShapeDtypeStruct((72, 128), jnp.float32), small, small),
        in_specs=vmem(4),
        out_specs=tuple(vmem(3)),
        compiler_params=pltpu.CompilerParams(vmem_limit_bytes=2 * 1024 * 1024),
        cost_estimate=pl.CostEstimate(flops=200000, bytes_accessed=200000, transcendentals=0),
        name="edge",
    )(from_left, from_right, from_low, from_high)
    edges_below = sent(edges, "gz", 1)
    edges_above = sent(edges, "gz", -1)
    corner_left = sent(right, "gx", 1)
    corner_right = sent(left, "gx", -1)
    next_section, result, rates = pl.pallas_call(
        rate_kernel,
        out_shape=(block, block, block),
        in_specs=vmem(12),
        out_specs=tuple(vmem(3)),
        scratch_shapes=[
            pltpu.VMEM((25, 6, 32, 128), jnp.float32),
            pltpu.VMEM((25, 2, 16, 128), jnp.float32),
            pltpu.VMEM((5, 6, 32, 128), jnp.float32),
            pltpu.VMEM((5, 6, 16, 128), jnp.float32),
        ],
        compiler_params=pltpu.CompilerParams(vmem_limit_bytes=16 * 1024 * 1024),
        cost_estimate=pl.CostEstimate(flops=30000000, bytes_accessed=3000000, transcendentals=0),
        name="rate",
    )(
        held,
        below,
        above,
        from_left,
        from_right,
        from_low,
        from_high,
        edges_below,
        edges_above,
        corner_left,
        corner_right,
        base,
    )
    next_accum = pl.pallas_call(
        tally_kernel,
        out_shape=block,
        in_specs=vmem(2),
        out_specs=vmem(1)[0],
        compiler_params=pltpu.CompilerParams(vmem_limit_bytes=4 * 1024 * 1024),
        cost_estimate=pl.CostEstimate(flops=200000, bytes_accessed=1300000, transcendentals=0),
        name="tally",
    )(accum, rates)
    return (next_section, next_accum, slab_of(result))


def solution(mesh):
    split = P(None, "gz", "gy", "gx")
    return jax.shard_map(
        shards,
        mesh=mesh,
        in_specs=(split, split, split),
        out_specs=(split, split, P(None, "gz", None, None)),
        check_vma=False,
    )
```
